32 devices in a mesh: px: 4 (over z), py: 4 (over y, x), pz: 2 (over core).
Axes of the slice: x: 2, y: 2, z: 4, core: 2. Of those that a mesh axis runs over, the one named last changes fastest.
Arguments:
- right_side: float32 [16, 64, 256], P('px', 'py', 'pz'), may hold values from -160 to 160
- start_guess: float32 [16, 64, 256], P('px', 'py', 'pz'), may hold values from -4 to 4
- conductivity: float32 [16, 64, 256], P('px', 'py', 'pz'), may hold values from 0.05 to 0.4
- recycled: float32 [16, 16, 64, 256], P(None, 'px', 'py', 'pz'), may hold values from -6 to 6
Outputs:
- solution: float32 [16, 64, 256], P('px', 'py', 'pz')
- residual: float32 [16, 64, 256], P('px', 'py', 'pz')
- hessenberg: float32 [9, 8], replicated
The draws below stay inside these ranges and needn't reach their ends.
All inputs are finite; a program needn't handle non-finite values.
Results may differ from the reference program's by a relative error of at most 0.03.
Values sent between devices are 32-bit elements; how exact they have to be, the bound alone decides.
A program may use at most 128 MiB of HBM per device.

```python
import math
import jax
import jax.numpy as jnp
from jax import lax

K = 16
STEPS = 8
NX = 16
NY = 64
NZ = 256


def recycled_fields(key):
    base_key = jax.random.fold_in(key, 11)
    return jnp.clip(jax.random.normal(base_key, (K, NX, NY, NZ), jnp.float32), -6.0, 6.0)


def draw_recycled(key, part):
    return recycled_fields(key)


def draw_right_side(key, part):
    fields = recycled_fields(key)
    weights = 0.5 * jnp.clip(jax.random.normal(jax.random.fold_in(key, 12), (K,), jnp.float32), -3.0, 3.0)
    noise_part = jnp.clip(jax.random.normal(jax.random.fold_in(key, 13), (NX, NY, NZ), jnp.float32), -6.0, 6.0)
    combined = noise_part + jnp.tensordot(weights, fields, axes=1)
    return combined


def level_of(rng, extent, pieces, low, largest):
    def one(dim, parts):
        heights = jax.random.uniform(jax.random.fold_in(jax.random.fold_in(rng, 6), dim), (parts,), jnp.float32, low / len(pieces), largest / len(pieces))
        return jnp.repeat(jnp.exp(heights), extent[dim] // parts).reshape((-1,) + (1,) * (len(extent) - dim - 1))

    loudness = one(*pieces[0])
    for cut in pieces[1:]:
        loudness = loudness * one(*cut)
    return loudness


def bell_draw(stream_key, dims, deviation, reach, pieces=(), kind=jnp.bfloat16):
    entries = deviation * jax.random.normal(stream_key, dims, jnp.float32)
    if pieces:
        entries = entries * level_of(stream_key, dims, pieces, -0.22, 0.18)
    return jnp.clip(entries, -reach, reach).astype(kind)


def setup_inputs(seed: int = 0) -> dict:
    key_of = jax.random.split(jax.random.key(seed), 5)
    right_side = draw_right_side(jax.random.fold_in(key_of[4], 71), 0)
    start_guess = bell_draw(key_of[1], (NX, NY, NZ), 0.3, 4.0, ((0, 4), (1, 4), (2, 2)), jnp.float32)
    conductivity = jnp.clip(jnp.exp(math.log(0.4) - 2.0794415 * jax.random.uniform(key_of[2], (NX, NY, NZ), jnp.float32) ** level_of(key_of[2], (NX, NY, NZ), ((0, 4), (1, 4), (2, 2)), -0.2, 0.2)), 0.05, 0.4)
    recycled = draw_recycled(jax.random.fold_in(key_of[4], 71), 0)
    return dict(right_side=right_side, start_guess=start_guess, conductivity=conductivity, recycled=recycled)


highest = lax.Precision.HIGHEST
edge_weight = 0.25 ** (1.0 / 3.0)
middle_weight = 2.0 * edge_weight
shift_value = 0.4

def stencil_sum(padded):
    along_z = edge_weight * (padded[..., :-2] + padded[..., 2:]) + middle_weight * padded[..., 1:-1]
    along_y = edge_weight * (along_z[..., :-2, :] + along_z[..., 2:, :]) + middle_weight * along_z[..., 1:-1, :]
    along_x = edge_weight * (along_y[..., :-2, :, :] + along_y[..., 2:, :, :]) + middle_weight * along_y[..., 1:-1, :, :]
    return along_x - 2.0 * padded[..., 1:-1, 1:-1, 1:-1]

def pad_cells(field_in):
    return jnp.pad(field_in, ((1, 1), (1, 1), (1, 1)))

def operate(field_in, conductivity, diagonal):
    near_sum = stencil_sum(pad_cells(field_in))
    far_sum = stencil_sum(pad_cells(conductivity * field_in))
    return diagonal * field_in - 0.5 * conductivity * near_sum - 0.5 * far_sum

def cholesky_low(gram):
    order = gram.shape[0]
    rows_idx = jnp.arange(order)
    factor = jnp.zeros((order, order), jnp.float32)
    for column in range(order):
        known = factor[:, :column]
        partial_sum = lax.optimization_barrier(jnp.sum(known * known[column][None, :], axis=1))
        pivot = jnp.sqrt(gram[column, column] - partial_sum[column])
        values = (gram[:, column] - partial_sum) / pivot
        values = jnp.where(rows_idx > column, values, 0.0)
        factor = factor.at[:, column].set(values).at[column, column].set(pivot)
    return factor

def lower_inverse(factor):
    order = factor.shape[0]
    inverse = jnp.zeros((order, order), jnp.float32)
    for row in range(order):
        unit_row = jnp.zeros((order,), jnp.float32).at[row].set(1.0)
        partial_value = lax.optimization_barrier(jnp.sum(factor[row, :row][:, None] * inverse[:row], axis=0))
        inverse = inverse.at[row].set((unit_row - partial_value) / factor[row, row])
    return inverse

def back_solve(upper_tri, target):
    order = upper_tri.shape[0]
    result = jnp.zeros((order,), jnp.float32)
    for row in range(order - 1, -1, -1):
        partial_value = jnp.sum(upper_tri[row, row + 1:] * result[row + 1:])
        result = result.at[row].set((target[row] - partial_value) / upper_tri[row, row])
    return result

def least_squares(hessenberg, beta_norm):
    upper_tri = hessenberg
    target = jnp.zeros((STEPS + 1,), jnp.float32).at[0].set(beta_norm)
    for column in range(STEPS):
        top_entry = upper_tri[column, column]
        low_entry = upper_tri[column + 1, column]
        radius = jnp.sqrt(top_entry * top_entry + low_entry * low_entry)
        cosine = top_entry / radius
        sine_val = low_entry / radius
        row_top = cosine * upper_tri[column] + sine_val * upper_tri[column + 1]
        row_low = cosine * upper_tri[column + 1] - sine_val * upper_tri[column]
        upper_tri = upper_tri.at[column].set(row_top).at[column + 1].set(row_low)
        goal_top = cosine * target[column] + sine_val * target[column + 1]
        goal_low = cosine * target[column + 1] - sine_val * target[column]
        target = target.at[column].set(goal_top).at[column + 1].set(goal_low)
    return back_solve(upper_tri[:STEPS], target[:STEPS])

def reference(right_side, start_guess, conductivity, recycled):
    diagonal = shift_value + 7.0 * conductivity + 0.5 * stencil_sum(pad_cells(conductivity))
    images_c = lax.map(lambda single_field: operate(single_field, conductivity, diagonal), recycled)
    flat_images = images_c.reshape(K, -1)
    first_residual = (right_side - operate(start_guess, conductivity, diagonal)).reshape(-1)
    gram = jnp.dot(flat_images, flat_images.T, precision=highest)
    factor_low = cholesky_low(gram)
    inverse = lower_inverse(factor_low)
    basis_c = jnp.dot(inverse, flat_images, precision=highest)
    projected = jnp.dot(basis_c, first_residual, precision=highest)
    recycle_flat = recycled.reshape(K, -1)
    solution = start_guess.reshape(-1) + jnp.dot(jnp.dot(inverse.T, projected, precision=highest), recycle_flat, precision=highest)
    residual = first_residual - jnp.dot(projected, basis_c, precision=highest)
    beta_norm = jnp.sqrt(jnp.dot(residual, residual, precision=highest))
    krylov = [residual / beta_norm]
    coupling = jnp.zeros((K, STEPS), jnp.float32)
    hessenberg = jnp.zeros((STEPS + 1, STEPS), jnp.float32)
    for column in range(STEPS):
        vector_new = operate(krylov[column].reshape(NX, NY, NZ), conductivity, diagonal).reshape(-1)
        known_basis = jnp.stack(krylov)
        coeff_c = jnp.dot(basis_c, vector_new, precision=highest)
        coeff_v = jnp.dot(known_basis, vector_new, precision=highest)
        vector_new = vector_new - jnp.dot(coeff_c, basis_c, precision=highest) - jnp.dot(coeff_v, known_basis, precision=highest)
        norm_new = jnp.sqrt(jnp.dot(vector_new, vector_new, precision=highest))
        coupling = coupling.at[:, column].set(coeff_c)
        hessenberg = hessenberg.at[:column + 1, column].set(coeff_v)
        hessenberg = hessenberg.at[column + 1, column].set(norm_new)
        krylov.append(vector_new / norm_new)
    coeffs = least_squares(hessenberg, beta_norm)
    basis_all = jnp.stack(krylov)
    recycle_coeffs = jnp.dot(inverse.T, jnp.dot(coupling, coeffs, precision=highest), precision=highest)
    solution = solution + jnp.dot(coeffs, basis_all[:STEPS], precision=highest) - jnp.dot(recycle_coeffs, recycle_flat, precision=highest)
    residual = residual - jnp.dot(jnp.dot(hessenberg, coeffs, precision=highest), basis_all, precision=highest)
    return (solution.reshape(NX, NY, NZ), residual.reshape(NX, NY, NZ), hessenberg)
```

```python
import functools
import itertools

import jax
import jax.numpy as jnp
from jax import lax
from jax.experimental import pallas as pl
from jax.experimental.pallas import tpu as pltpu
from jax.sharding import PartitionSpec as P

STEPS = 8
MESH = pl.DeviceIdType.MESH
AXES = ("px", "py", "pz")
GROUPS = (("py", "pz"), ("px",))

edge_weight = 0.25 ** (1.0 / 3.0)
middle_weight = 2.0 * edge_weight
shift_value = 0.4

DIRS = [d for d in itertools.product((-1, 0, 1), repeat=3) if d != (0, 0, 0)]


def kernel(
    sizes,
    rhs, guess, cond, rec,
    sol_out, res_out, hes_out,
    src, img, bface, bedge, pack, pface, pedge,
    bx, by, bc,
    zm, zx, zy, zc,
    mx, my, mc,
    wbuf, wface, wedge,
    fields, kext, diag, temp, zext,
    gpart, gred1, gred2, sred1, sred2,
    mat, hcols, scale, coef, ecoef,
    hsend, hrecv, rsend, rrecv,
):
    nsz = dict(zip(AXES, sizes))
    me = {a: lax.axis_index(a) for a in AXES}
    K, X, Y, Z = rec.shape
    NF = K + 2
    C0 = K
    f32 = jnp.float32
    lane3 = lax.broadcasted_iota(jnp.int32, (X + 2, Y + 8, Z), 2)
    lane2 = lax.broadcasted_iota(jnp.int32, (32, Z), 1)
    row2 = lax.broadcasted_iota(jnp.int32, (32, Z), 0)

    def exists(d):
        ok = None
        for a, s in zip(AXES, d):
            if s == 0:
                continue
            here = (me[a] < nsz[a] - 1) if s > 0 else (me[a] > 0)
            ok = here if ok is None else jnp.logical_and(ok, here)
        return ok

    def possible(d):
        return all(s == 0 or nsz[a] > 1 for a, s in zip(AXES, d))

    dirs = [(i, d) for i, d in enumerate(DIRS) if possible(d)]

    def target(d):
        return tuple(me[a] + s for a, s in zip(AXES, d))

    def group_info(g):
        n = 1
        rank = 0
        for a in GROUPS[g]:
            n *= nsz[a]
            rank = rank * nsz[a] + me[a]
        return n, rank

    def member(g, r):
        co = dict(me)
        for a in reversed(GROUPS[g]):
            co[a] = lax.rem(r, nsz[a])
            r = lax.div(r, nsz[a])
        return tuple(co[a] for a in AXES)

    def copies(sends, recvs, slot):
        out = []
        for i, (dx, dy, dz) in dirs:
            main, face, edge = sends(dz)
            rm, rx, ry, rc = recvs(-dz)
            hx, hy = int(dx > 0), int(dy > 0)
            if dx == 0 and dy == 0:
                s, t = main, rm
            elif dy == 0:
                s, t = main.at[:, X - 1 if hx else 0], rx.at[1 - hx]
            elif dx == 0:
                s, t = face.at[hy], ry.at[1 - hy]
            else:
                s, t = edge.at[hx, hy], rc.at[1 - hx, 1 - hy]
            d = (dx, dy, dz)
            out.append((d, pltpu.make_async_remote_copy(
                src_ref=s, dst_ref=t,
                send_sem=hsend.at[slot, i], recv_sem=hrecv.at[slot, i],
                device_id=target(d), device_id_type=MESH,
            )))
        return out

    def start_halo(cs):
        for d, c in cs:
            pl.when(exists(d))(c.start)

    def wait_recv(cs):
        for d, c in cs:
            pl.when(exists(tuple(-s for s in d)))(c.wait_recv)

    def wait_send(cs):
        for d, c in cs:
            pl.when(exists(d))(c.wait_send)

    def batch_copies(b):
        def sends(dz):
            if dz == 0:
                return (src if b == 0 else img), bface.at[b], bedge.at[b]
            h = int(dz > 0)
            return pack.at[b, h], pface.at[b, h], pedge.at[b, h]

        def recvs(z):
            if z == 0:
                return None, bx.at[b], by.at[b], bc.at[b]
            h = int(z > 0)
            return zm.at[b, h], zx.at[b, h], zy.at[b, h], zc.at[b, h]

        return copies(sends, recvs, b)

    def step_copies(par):
        def sends(dz):
            return wbuf.at[par], wface.at[par], wedge.at[par]

        def recvs(z):
            if z == 0:
                return None, mx.at[par], my.at[par], mc.at[par]
            h = int(z > 0)
            return zm.at[2 + par, h], zx.at[2 + par, h], zy.at[2 + par, h], zc.at[2 + par, h]

        return copies(sends, recvs, 2 + par)

    def pack_faces(val, face, edge, row, erow):
        for h, y in ((0, 0), (1, Y - 1)):
            for x in range(X):
                face[h, pl.ds(row + x, 1), :] = val[x, y : y + 1, :]
            edge[0, h, pl.ds(erow, 1), :] = val[0, y : y + 1, :]
            edge[1, h, pl.ds(erow, 1), :] = val[X - 1, y : y + 1, :]

    def assemble(dst, main, rx, ry, rc, f, row, erow):
        dst[1 : X + 1, 0:Y, :] = main
        dst[0, 0:Y, :] = rx[0, f]
        dst[X + 1, 0:Y, :] = rx[1, f]
        for h, y in ((1, Y), (0, Y + 7)):
            for x in range(X):
                dst[1 + x, y : y + 1, :] = ry[h, pl.ds(row + x, 1), :]
            dst[0, y : y + 1, :] = rc[0, h, pl.ds(erow, 1), :]
            dst[X + 1, y : y + 1, :] = rc[1, h, pl.ds(erow, 1), :]

    def assemble_zones(slot):
        for h in range(2):
            assemble(zext.at[h], zm[slot, h, 0], zx.at[slot, h], zy.at[slot, h], zc.at[slot, h], 0, 0, 0)

    def zone_field(f):
        low = pltpu.roll(zext[0], lax.rem(2 * Z - 1 - f, Z), 2)
        high = pltpu.roll(zext[1], lax.rem(Z - f, Z), 2)
        return jnp.where(lane3 == Z - 1, low, jnp.where(lane3 == 0, high, 0.0))

    def pack_lanes(get, count, b):
        lane = lax.broadcasted_iota(jnp.int32, (X, Y, Z), 2)
        low = jnp.zeros((X, Y, Z), f32)
        high = jnp.zeros((X, Y, Z), f32)
        for f in range(count):
            v = get(f)
            low = jnp.where(lane == f, pltpu.roll(v, f, 2) if f else v, low)
            high = jnp.where(lane == f, pltpu.roll(v, (f + 1) % Z, 2), high)
        for h, v in ((0, low), (1, high)):
            pack[b, h, 0] = v
            pack_faces(v, pface.at[b, h], pedge.at[b, h], 0, 0)

    def stencil(e, b):
        left = pltpu.roll(jnp.where(lane3 == Z - 1, b, e), 1, 2)
        right = pltpu.roll(jnp.where(lane3 == 0, b, e), Z - 1, 2)
        az = edge_weight * (left + right) + middle_weight * e
        ay = edge_weight * (pltpu.roll(az, 1, 1) + pltpu.roll(az, Y + 7, 1)) + middle_weight * az
        ay = ay[:, :Y]
        ax = edge_weight * (ay[:X] + ay[2:]) + middle_weight * ay[1 : X + 1]
        return ax - 2.0 * e[1 : X + 1, :Y]

    def apply(e, b):
        k = kext[0]
        near = stencil(e, b)
        far = stencil(k * e, kext[1] * b)
        return diag[...] * e[1 : X + 1, :Y] - 0.5 * k[1 : X + 1, :Y] * near - 0.5 * far

    def tile_sum(v):
        v = jnp.sum(v.reshape(X * Y // 8, 8, Z), axis=0)
        return jnp.sum(v, axis=0, keepdims=True)

    def all_reduce(value, bufs, slot):
        total = value
        for g in range(len(GROUPS)):
            n, rank = group_info(g)
            buf = bufs[g]
            buf[rank] = total
            cs = []
            for k in range(1, n):
                c = pltpu.make_async_remote_copy(
                    src_ref=buf.at[rank], dst_ref=buf.at[rank],
                    send_sem=rsend.at[slot, g, k], recv_sem=rrecv.at[slot, g, k],
                    device_id=member(g, lax.rem(rank + k, n)), device_id_type=MESH,
                )
                c.start()
                cs.append((k, c))
            for k, c in cs:
                pltpu.make_async_remote_copy(
                    src_ref=buf.at[rank], dst_ref=buf.at[lax.rem(rank + n - k, n)],
                    send_sem=rsend.at[slot, g, k], recv_sem=rrecv.at[slot, g, k],
                    device_id=member(g, lax.rem(rank + k, n)), device_id_type=MESH,
                ).wait_recv()
            total = buf[0]
            for r in range(1, n):
                total = total + buf[r]
            for k, c in cs:
                c.wait_send()
        return total

    for ref in (bx, by, bc, zm, zx, zy, zc, mx, my, mc, wface, wedge, bface, bedge, pface, pedge):
        lead = ref.shape[0]

        def clear(i, carry, ref=ref):
            ref[i] = jnp.zeros(ref.shape[1:], f32)
            return carry

        lax.fori_loop(0, lead, clear, 0)

    def clear_fields(i, carry):
        fields[i] = jnp.zeros(fields.shape[1:], f32)
        return carry

    lax.fori_loop(0, fields.shape[0], clear_fields, 0)
    kext[...] = jnp.zeros(kext.shape, f32)
    temp[...] = jnp.zeros(temp.shape, f32)
    zext[...] = jnp.zeros(zext.shape, f32)
    img[NF - 1] = jnp.zeros((X, Y, Z), f32)

    def load_field(f, carry):
        v = rec[f]
        src[f] = v
        pack_faces(v, bface.at[0], bedge.at[0], f * X, f)
        return carry

    lax.fori_loop(0, K, load_field, 0)
    for f, ref in ((K, guess), (K + 1, cond)):
        v = ref[...]
        src[f] = v
        pack_faces(v, bface.at[0], bedge.at[0], f * X, f)
    pack_lanes(lambda f: src[f], NF, 0)

    barrier = pltpu.get_barrier_semaphore()
    count = jnp.int32(0)
    for _, d in dirs:
        ok = exists(d)

        @pl.when(ok)
        def _(d=d):
            pl.semaphore_signal(barrier, inc=1, device_id=target(d), device_id_type=MESH)

        count = count + ok.astype(jnp.int32)
    for g in range(len(GROUPS)):
        n, rank = group_info(g)
        for k in range(1, n):
            pl.semaphore_signal(
                barrier, inc=1, device_id=member(g, lax.rem(rank + k, n)), device_id_type=MESH
            )
        count = count + (n - 1)
    pl.semaphore_wait(barrier, count)

    first = batch_copies(0)
    start_halo(first)
    wait_recv(first)
    assemble_zones(0)
    assemble(kext.at[0], src[K + 1], bx.at[0], by.at[0], bc.at[0], K + 1, (K + 1) * X, K + 1)
    kext[1] = zone_field(K + 1)
    k_all = kext[0]
    diag[...] = shift_value + 7.0 * k_all[1 : X + 1, :Y] + 0.5 * stencil(k_all, kext[1])

    def image(f, carry):
        assemble(temp, src[f], bx.at[0], by.at[0], bc.at[0], f, f * X, f)
        v = apply(temp[...], zone_field(f))
        img[f] = v
        return carry

    lax.fori_loop(0, K + 1, image, 0)
    img[K] = rhs[...] - img[K]

    def face_image(f, carry):
        pack_faces(img[f], bface.at[1], bedge.at[1], f * X, f)
        return carry

    lax.fori_loop(0, K + 1, face_image, 0)
    pack_lanes(lambda f: img[f], K + 1, 1)
    second = batch_copies(1)
    start_halo(second)

    GR = gpart.shape[1]

    def gram_part(a, carry):
        va = img[a]
        rows = [tile_sum(img[b] * va) for b in range(K + 1)]
        rows.append(jnp.zeros((GR - K - 1, Z), f32))
        gpart[a] = jnp.concatenate(rows, axis=0)
        return carry

    lax.fori_loop(0, K + 1, gram_part, 0)
    lane_g = lax.broadcasted_iota(jnp.int32, (GR, Z), 1)
    gram = jnp.zeros((GR, Z), f32)
    for a in range(K + 1):
        gram = jnp.where(lane_g == a, jnp.sum(gpart[a], axis=1, keepdims=True), gram)
    gram = all_reduce(gram, (gred1, gred2), 2)

    lane_k = lax.broadcasted_iota(jnp.int32, (K, Z), 1)
    row_k = lax.broadcasted_iota(jnp.int32, (K, Z), 0)
    a_mat = jnp.where(lane_k < K, gram[:K], 0.0)
    for k in range(K):
        prow = a_mat[k : k + 1, :]
        pcol = a_mat[:, k : k + 1]
        inv_p = 1.0 / a_mat[k : k + 1, k : k + 1]
        prow_s = jnp.where(lax.broadcasted_iota(jnp.int32, (1, Z), 1) == k, 1.0, prow) * inv_p
        base = jnp.where(lane_k == k, 0.0, a_mat)
        a_mat = jnp.where(row_k == k, jnp.broadcast_to(prow_s, (K, Z)), base - pcol * prow_s)
    mat[...] = jnp.where(lane2 == row2, 1.0, 0.0)
    mat[0:K, :] = a_mat
    grow = jnp.where(lax.broadcasted_iota(jnp.int32, (1, Z), 1) < K, gram[K : K + 1, :], 0.0)
    ecoef[...] = jnp.broadcast_to(jnp.sum(a_mat * grow, axis=1, keepdims=True), (K, Z))

    wait_recv(second)
    assemble_zones(1)

    def extend(f, carry):
        assemble(fields.at[f, 0], img[f], bx.at[1], by.at[1], bc.at[1], f, f * X, f)
        fields[f, 1] = zone_field(f)
        return carry

    lax.fori_loop(0, K + 1, extend, 0)

    def begin(p, carry):
        z, x = lax.div(p, X + 2), lax.rem(p, X + 2)
        v = fields[C0, z, x]
        for a in range(K):
            v = v - ecoef[a : a + 1, :] * fields[a, z, x]
        fields[C0, z, x] = v
        return carry

    lax.fori_loop(0, 2 * (X + 2), begin, 0)
    wait_send(first)
    wait_send(second)
    hcols[...] = jnp.zeros((32, Z), f32)
    scale[...] = jnp.where(row2 < K, 1.0, 0.0)

    def step(j, carry):
        par = lax.rem(j, 2)
        u = fields[C0 + j, 0]
        w = apply(u, fields[C0 + j, 1])
        wbuf[par, 0] = w
        pack_faces(w, wface.at[par], wedge.at[par], 0, 0)
        cs = step_copies(par)

        @pl.when(j < STEPS - 1)
        def _():
            start_halo(cs)

        rows = [tile_sum(fields[f, 0, 1 : X + 1, 0:Y, :] * w) for f in range(K + STEPS)]
        ui = u[1 : X + 1, :Y]
        rows.append(tile_sum(w * w))
        rows.append(tile_sum(ui * ui))
        rows.append(jnp.zeros((32 - K - STEPS - 2, Z), f32))
        sums = jnp.sum(jnp.concatenate(rows, axis=0), axis=1, keepdims=True)
        part = jnp.sum(jnp.where(lane2 == row2, sums, 0.0), axis=0, keepdims=True)
        total = all_reduce(jnp.broadcast_to(part, (8, Z)), (sred1.at[par], sred2.at[par]), par)
        total = jnp.concatenate([total] * 4, axis=0)
        c = jnp.broadcast_to(jnp.sum(mat[...] * total, axis=1, keepdims=True), (32, Z))
        uu = c[K + STEPS + 1 : K + STEPS + 2, :]
        sc = jnp.where(row2 == C0 + j, 1.0 / uu, scale[...])
        scale[...] = sc
        hcols[...] = jnp.where(lane2 == j, c, hcols[...])
        inv_n = 1.0 / jnp.sqrt(uu)
        coef[...] = jnp.where(
            row2 < K + STEPS, c * sc * inv_n, jnp.where(row2 == 30, inv_n, total)
        )

        @pl.when(j < STEPS - 1)
        def _():
            wait_recv(cs)
            slot = 2 + par
            assemble(temp, wbuf[par, 0], mx.at[par], my.at[par], mc.at[par], 0, 0, 0)
            fields[C0 + 1 + j, 0] = temp[...]
            assemble_zones(slot)
            fields[C0 + 1 + j, 1] = jnp.where(
                lane3 == Z - 1, zext[0], jnp.where(lane3 == 0, zext[1], 0.0)
            )

        @pl.when(j == STEPS - 1)
        def _():
            fields[C0 + STEPS, 0, 1 : X + 1, 0:Y, :] = wbuf[par, 0]

        def update(p, carry):
            z, x = lax.div(p, X + 2), lax.rem(p, X + 2)
            v = coef[30:31, :] * fields[C0 + 1 + j, z, x]
            v2 = jnp.zeros_like(v)
            for a in range(0, K + STEPS, 2):
                v = v - coef[a : a + 1, :] * fields[a, z, x]
                v2 = v2 - coef[a + 1 : a + 2, :] * fields[a + 1, z, x]
            fields[C0 + 1 + j, z, x] = v + v2
            return carry

        lax.fori_loop(0, 2 * (X + 2), update, 0)

        @pl.when(j < STEPS - 1)
        def _():
            wait_send(cs)

        return carry

    lax.fori_loop(0, STEPS, step, 0)

    lane8 = lane2[:8]
    row8 = row2[:8]
    hc = hcols[...]
    inv_n2 = scale[C0 : C0 + STEPS, :]
    inv_col = jnp.sqrt(inv_n2)
    n_col = 1.0 / inv_col
    inv_row = jnp.sum(jnp.where(lane8 == row8, inv_col, 0.0), axis=0, keepdims=True)
    last_c = jnp.sum(jnp.where(lane2 == STEPS - 1, hc, 0.0), axis=1, keepdims=True)
    raw = jnp.broadcast_to(coef[31:32, :], (32, Z))
    raw_col = jnp.sum(jnp.where(lane2 == row2, raw, 0.0), axis=1, keepdims=True)
    terms = jnp.where(row2[:, :1] < K + STEPS, raw_col * last_c * scale[:, :1], 0.0)
    used = jnp.sum(terms, axis=0, keepdims=True)
    last_sq = (raw_col[K + STEPS : K + STEPS + 1] - used) * inv_n2[STEPS - 1 : STEPS, :1]
    last_n = jnp.sqrt(last_sq)
    upper = hc[C0 : C0 + STEPS] * inv_col * inv_row
    upper = jnp.where(lane8 < STEPS, upper, 0.0)
    upper = jnp.where(lane8 == row8 - 1, n_col, upper)
    lane1 = lane2[:1]
    bottom = jnp.where(lane1 == STEPS - 1, last_n, 0.0)
    hes = jnp.concatenate([upper, bottom], axis=0)
    hes_out[...] = hes[:, :STEPS]

    rows = [hes[i : i + 1] for i in range(STEPS + 1)]
    rows[0] = jnp.where(lane1 == STEPS, n_col[0:1], rows[0])
    for i in range(STEPS):
        top, low = rows[i][:, i : i + 1], rows[i + 1][:, i : i + 1]
        inv_r = 1.0 / jnp.sqrt(top * top + low * low)
        cs_, sn = top * inv_r, low * inv_r
        rows[i], rows[i + 1] = cs_ * rows[i] + sn * rows[i + 1], cs_ * rows[i + 1] - sn * rows[i]
    ysol = jnp.zeros((1, Z), f32)
    for i in range(STEPS - 1, -1, -1):
        known = jnp.sum(jnp.where(lane1 > i, rows[i] * ysol, 0.0), axis=1, keepdims=True)
        yi = (rows[i][:, STEPS : STEPS + 1] - known) / rows[i][:, i : i + 1]
        ysol = jnp.where(lane1 == i, yi, ysol)

    rcoef = ecoef[:, :1] - jnp.sum(hc[:K] * (ysol * inv_row), axis=1, keepdims=True)
    ycol = jnp.sum(jnp.where(lane8 == row8, ysol * inv_row, 0.0), axis=1, keepdims=True)
    hy8 = jnp.sum(upper * ysol, axis=1, keepdims=True) * inv_col[:, :1]
    hy9 = jnp.sum(bottom * ysol, axis=1, keepdims=True) / last_n
    out = guess[...]
    for a in range(K):
        out = out + rcoef[a : a + 1, :] * rec[a]
    res = fields[C0, 0, 1 : X + 1, 0:Y, :]
    for i in range(STEPS):
        ui = fields[C0 + i, 0, 1 : X + 1, 0:Y, :]
        out = out + ycol[i : i + 1, :] * ui
        res = res - hy8[i : i + 1, :] * ui
    res = res - hy9 * fields[C0 + STEPS, 0, 1 : X + 1, 0:Y, :]
    sol_out[...] = out
    res_out[...] = res


def round_up(n, m):
    return (n + m - 1) // m * m


def solution(mesh):
    sizes = tuple(mesh.shape[a] for a in AXES)

    def body(right_side, start_guess, conductivity, recycled):
        K, X, Y, Z = recycled.shape
        NF = K + 2
        FR, ER, XR = round_up(NF * X, 8), round_up(NF, 8), round_up(X, 8)
        groups = []
        for g in GROUPS:
            n = 1
            for a in g:
                n *= mesh.shape[a]
            groups.append(n)
        biggest = max(groups)
        GR = round_up(K + 1, 8)
        V = lambda *s: pltpu.VMEM(s, jnp.float32)
        vm = pl.BlockSpec(memory_space=pltpu.VMEM)
        shape = jax.ShapeDtypeStruct((X, Y, Z), jnp.float32)
        return pl.pallas_call(
            functools.partial(kernel, sizes),
            out_shape=(shape, shape, jax.ShapeDtypeStruct((STEPS + 1, STEPS), jnp.float32)),
            in_specs=[vm] * 4,
            out_specs=(vm, vm, vm),
            scratch_shapes=[
                V(NF, X, Y, Z), V(NF, X, Y, Z),
                V(2, 2, FR, Z), V(2, 2, 2, ER, Z),
                V(2, 2, 1, X, Y, Z), V(2, 2, 2, XR, Z), V(2, 2, 2, 2, 8, Z),
                V(2, 2, NF, Y, Z), V(2, 2, FR, Z), V(2, 2, 2, ER, Z),
                V(4, 2, 1, X, Y, Z), V(4, 2, 2, 1, Y, Z), V(4, 2, 2, XR, Z), V(4, 2, 2, 2, 8, Z),
                V(2, 2, 1, Y, Z), V(2, 2, XR, Z), V(2, 2, 2, 8, Z),
                V(2, 1, X, Y, Z), V(2, 2, XR, Z), V(2, 2, 2, 8, Z),
                V(K + STEPS + 1, 2, X + 2, Y + 8, Z), V(2, X + 2, Y + 8, Z), V(X, Y, Z),
                V(X + 2, Y + 8, Z), V(2, X + 2, Y + 8, Z),
                V(K + 1, GR, Z), V(groups[0], GR, Z), V(groups[1], GR, Z),
                V(2, groups[0], 8, Z), V(2, groups[1], 8, Z),
                V(32, Z), V(32, Z), V(32, Z), V(32, Z), V(K, Z),
                pltpu.SemaphoreType.DMA((4, 26)), pltpu.SemaphoreType.DMA((4, 26)),
                pltpu.SemaphoreType.DMA((3, 2, biggest)), pltpu.SemaphoreType.DMA((3, 2, biggest)),
            ],
            compiler_params=pltpu.CompilerParams(collective_id=0, has_side_effects=True),
        )(right_side, start_guess, conductivity, recycled)

    return jax.shard_map(
        body,
        mesh=mesh,
        in_specs=(P(*AXES), P(*AXES), P(*AXES), P(None, *AXES)),
        out_specs=(P(*AXES), P(*AXES), P()),
        check_vma=False,
    )
```

```python
import functools
import itertools

import jax
import jax.numpy as jnp
from jax import lax
from jax.experimental import pallas as pl
from jax.experimental.pallas import tpu as pltpu
from jax.sharding import PartitionSpec as P

STEPS = 8
MESH = pl.DeviceIdType.MESH
AXES = ("px", "py", "pz")
TWO = (("py", "pz"), ("px",))
ONE = (("px", "py", "pz"),)
CHUNK = 8

edge_weight = 0.25 ** (1.0 / 3.0)
middle_weight = 2.0 * edge_weight
shift_value = 0.4

DIRS = [d for d in itertools.product((-1, 0, 1), repeat=3) if d != (0, 0, 0)]


def kernel(
    sizes, groups,
    rhs, guess, cond, rec,
    sol_out, res_out, hes_out,
    src, img, bface, bedge, pack, pface, pedge,
    bx, by, bc,
    zm, zx, zy, zc,
    mx, my, mc,
    wbuf, wface, wedge,
    fields, kext, diag, temp, zext,
    gpart, gred1, gred2, sred1, sred2,
    mat, hcols, scale, coef, ecoef,
    hsend, hrecv, rsend, rrecv,
):
    nsz = dict(zip(AXES, sizes))
    me = {a: lax.axis_index(a) for a in AXES}
    K, X, Y, Z = rec.shape
    NF = K + 2
    C0 = K
    f32 = jnp.float32
    lane3 = lax.broadcasted_iota(jnp.int32, (X + 2, Y + 8, Z), 2)
    lane2 = lax.broadcasted_iota(jnp.int32, (32, Z), 1)
    row2 = lax.broadcasted_iota(jnp.int32, (32, Z), 0)

    def exists(d):
        ok = None
        for a, s in zip(AXES, d):
            if s == 0:
                continue
            here = (me[a] < nsz[a] - 1) if s > 0 else (me[a] > 0)
            ok = here if ok is None else jnp.logical_and(ok, here)
        return ok

    def possible(d):
        return all(s == 0 or nsz[a] > 1 for a, s in zip(AXES, d))

    dirs = [(i, d) for i, d in enumerate(DIRS) if possible(d)]

    def target(d):
        return tuple(me[a] + s for a, s in zip(AXES, d))

    def group_info(group):
        n = 1
        rank = 0
        for a in group:
            n *= nsz[a]
            rank = rank * nsz[a] + me[a]
        return n, rank

    def member(group, r):
        co = dict(me)
        for a in reversed(group):
            co[a] = lax.rem(r, nsz[a])
            r = lax.div(r, nsz[a])
        return tuple(co[a] for a in AXES)

    def copies(sends, recvs, slot, zones):
        out = []
        for i, (dx, dy, dz) in dirs:
            if (dz != 0) not in zones:
                continue
            main, face, edge = sends(dz)
            rm, rx, ry, rc = recvs(-dz)
            hx, hy = int(dx > 0), int(dy > 0)
            if dx == 0 and dy == 0:
                s, t = main, rm
            elif dy == 0:
                s, t = main.at[:, X - 1 if hx else 0], rx.at[1 - hx]
            elif dx == 0:
                s, t = face.at[hy], ry.at[1 - hy]
            else:
                s, t = edge.at[hx, hy], rc.at[1 - hx, 1 - hy]
            d = (dx, dy, dz)
            out.append((d, pltpu.make_async_remote_copy(
                src_ref=s, dst_ref=t,
                send_sem=hsend.at[slot, i], recv_sem=hrecv.at[slot, i],
                device_id=target(d), device_id_type=MESH,
            )))
        return out

    def start_halo(cs):
        for d, c in cs:
            pl.when(exists(d))(c.start)

    def wait_recv(cs):
        for d, c in cs:
            pl.when(exists(tuple(-s for s in d)))(c.wait_recv)

    def wait_send(cs):
        for d, c in cs:
            pl.when(exists(d))(c.wait_send)

    NC = (NF + CHUNK - 1) // CHUNK

    def batch_copies(b, c):
        f0, f1 = c * CHUNK, min((c + 1) * CHUNK, NF)
        fs, es = pl.ds(f0, f1 - f0), pl.ds(f0, CHUNK)
        rows = pl.ds(f0 * X, min(CHUNK * X, bface.shape[2] - f0 * X))

        def sends(dz):
            if dz == 0:
                body = (src if b == 0 else img).at[fs]
                return body, bface.at[b, :, rows], bedge.at[b, :, :, es]
            h = int(dz > 0)
            return pack.at[b, h], pface.at[b, h], pedge.at[b, h]

        def recvs(z):
            if z == 0:
                return None, bx.at[b, :, fs], by.at[b, :, rows], bc.at[b, :, :, es]
            h = int(z > 0)
            return zm.at[b, h], zx.at[b, h], zy.at[b, h], zc.at[b, h]

        return copies(sends, recvs, b * (NC + 1) + c, (c == NC,))

    def step_copies(par):
        def sends(dz):
            return wbuf.at[par], wface.at[par], wedge.at[par]

        def recvs(z):
            if z == 0:
                return None, mx.at[par], my.at[par], mc.at[par]
            h = int(z > 0)
            return zm.at[2 + par, h], zx.at[2 + par, h], zy.at[2 + par, h], zc.at[2 + par, h]

        return copies(sends, recvs, 2 * (NC + 1) + par, (False, True))

    def pack_faces(val, face, edge, row, erow):
        for h, y in ((0, 0), (1, Y - 1)):
            for x in range(X):
                face[h, pl.ds(row + x, 1), :] = val[x, y : y + 1, :]
            edge[0, h, pl.ds(erow, 1), :] = val[0, y : y + 1, :]
            edge[1, h, pl.ds(erow, 1), :] = val[X - 1, y : y + 1, :]

    def assemble(dst, main, rx, ry, rc, f, row, erow):
        dst[1 : X + 1, 0:Y, :] = main
        dst[0, 0:Y, :] = rx[0, f]
        dst[X + 1, 0:Y, :] = rx[1, f]
        for h, y in ((1, Y), (0, Y + 7)):
            for x in range(X):
                dst[1 + x, y : y + 1, :] = ry[h, pl.ds(row + x, 1), :]
            dst[0, y : y + 1, :] = rc[0, h, pl.ds(erow, 1), :]
            dst[X + 1, y : y + 1, :] = rc[1, h, pl.ds(erow, 1), :]

    def assemble_zones(slot):
        for h in range(2):
            assemble(zext.at[h], zm[slot, h, 0], zx.at[slot, h], zy.at[slot, h], zc.at[slot, h], 0, 0, 0)

    def zone_field(f):
        low = pltpu.roll(zext[0], lax.rem(2 * Z - 1 - f, Z), 2)
        high = pltpu.roll(zext[1], lax.rem(Z - f, Z), 2)
        return jnp.where(lane3 == Z - 1, low, jnp.where(lane3 == 0, high, 0.0))

    def pack_lanes(get, count, b):
        lane = lax.broadcasted_iota(jnp.int32, (X, Y, Z), 2)
        low = jnp.zeros((X, Y, Z), f32)
        high = jnp.zeros((X, Y, Z), f32)
        for f in range(count):
            v = get(f)
            low = jnp.where(lane == f, pltpu.roll(v, f, 2) if f else v, low)
            high = jnp.where(lane == f, pltpu.roll(v, (f + 1) % Z, 2), high)
        for h, v in ((0, low), (1, high)):
            pack[b, h, 0] = v
            pack_faces(v, pface.at[b, h], pedge.at[b, h], 0, 0)

    def stencil(e, b):
        left = pltpu.roll(jnp.where(lane3 == Z - 1, b, e), 1, 2)
        right = pltpu.roll(jnp.where(lane3 == 0, b, e), Z - 1, 2)
        az = edge_weight * (left + right) + middle_weight * e
        ay = edge_weight * (pltpu.roll(az, 1, 1) + pltpu.roll(az, Y + 7, 1)) + middle_weight * az
        ay = ay[:, :Y]
        ax = edge_weight * (ay[:X] + ay[2:]) + middle_weight * ay[1 : X + 1]
        return ax - 2.0 * e[1 : X + 1, :Y]

    def apply(e, b):
        k = kext[0]
        near = stencil(e, b)
        far = stencil(k * e, kext[1] * b)
        return diag[...] * e[1 : X + 1, :Y] - 0.5 * k[1 : X + 1, :Y] * near - 0.5 * far

    def tile_sum(v):
        v = jnp.sum(v.reshape(X * Y // 8, 8, Z), axis=0)
        return jnp.sum(v, axis=0, keepdims=True)

    def all_reduce(value, groups, bufs, slot, between):
        total = value
        for g, group in enumerate(groups):
            n, rank = group_info(group)
            buf = bufs[g]
            buf[rank] = total
            cs = []
            for k in range(1, n):
                c = pltpu.make_async_remote_copy(
                    src_ref=buf.at[rank], dst_ref=buf.at[rank],
                    send_sem=rsend.at[slot, g, k], recv_sem=rrecv.at[slot, g, k],
                    device_id=member(group, lax.rem(rank + k, n)), device_id_type=MESH,
                )
                c.start()
                cs.append((k, c))
            if g == len(groups) - 1:
                between()
            for k, c in cs:
                pltpu.make_async_remote_copy(
                    src_ref=buf.at[rank], dst_ref=buf.at[lax.rem(rank + n - k, n)],
                    send_sem=rsend.at[slot, g, k], recv_sem=rrecv.at[slot, g, k],
                    device_id=member(group, lax.rem(rank + k, n)), device_id_type=MESH,
                ).wait_recv()
            total = buf[0]
            for r in range(1, n):
                total = total + buf[r]
            for k, c in cs:
                c.wait_send()
        return total

    def clear_all(refs):
        for ref in refs:
            def clear(i, carry, ref=ref):
                ref[i] = jnp.zeros(ref.shape[1:], f32)
                return carry

            lax.fori_loop(0, ref.shape[0], clear, 0)

    clear_all((bx, by, bc, zm, zx, zy, zc, mx, my, mc))
    barrier = pltpu.get_barrier_semaphore()
    count = jnp.int32(0)
    for _, d in dirs:
        ok = exists(d)

        @pl.when(ok)
        def _(d=d):
            pl.semaphore_signal(barrier, inc=1, device_id=target(d), device_id_type=MESH)

        count = count + ok.astype(jnp.int32)
    for group in sorted(set(TWO + groups)):
        n, rank = group_info(group)
        for k in range(1, n):
            pl.semaphore_signal(
                barrier, inc=1, device_id=member(group, lax.rem(rank + k, n)), device_id_type=MESH
            )
        count = count + (n - 1)

    clear_all((wface, wedge, bface, bedge, pface, pedge))

    def load_field(f, carry):
        v = rec[f]
        src[f] = v
        pack_faces(v, bface.at[0], bedge.at[0], f * X, f)
        return carry

    lax.fori_loop(0, K, load_field, 0)
    for f, ref in ((K, guess), (K + 1, cond)):
        v = ref[...]
        src[f] = v
        pack_faces(v, bface.at[0], bedge.at[0], f * X, f)
    pack_lanes(lambda f: src[f], NF, 0)
    pl.semaphore_wait(barrier, count)

    first = [batch_copies(0, c) for c in range(NC + 1)]
    second = [batch_copies(1, c) for c in range(NC + 1)]
    order = [NC - 1] + list(range(NC - 1))
    for c in [NC] + order:
        start_halo(first[c])
    clear_all((fields, kext, zext))
    temp[...] = jnp.zeros(temp.shape, f32)
    img[NF - 1] = jnp.zeros((X, Y, Z), f32)
    wait_recv(first[NC])
    assemble_zones(0)

    def image(f, carry):
        assemble(temp, src[f], bx.at[0], by.at[0], bc.at[0], f, f * X, f)
        v = apply(temp[...], zone_field(f))
        img[f] = v
        pack_faces(v, bface.at[1], bedge.at[1], f * X, f)
        return carry

    for c in order:
        wait_recv(first[c])
        if c == NC - 1:
            assemble(kext.at[0], src[K + 1], bx.at[0], by.at[0], bc.at[0], K + 1, (K + 1) * X, K + 1)
            kext[1] = zone_field(K + 1)
            k_all = kext[0]
            diag[...] = shift_value + 7.0 * k_all[1 : X + 1, :Y] + 0.5 * stencil(k_all, kext[1])
            lax.fori_loop(c * CHUNK, K + 1, image, 0)
            v = rhs[...] - img[K]
            img[K] = v
            pack_faces(v, bface.at[1], bedge.at[1], K * X, K)
        else:
            lax.fori_loop(c * CHUNK, (c + 1) * CHUNK, image, 0)
        start_halo(second[c])
    pack_lanes(lambda f: img[f], K + 1, 1)
    start_halo(second[NC])

    GR = gpart.shape[1]
    GW = Z // (GR // 8)
    assert K + 1 <= GW

    def gram_part(a, carry):
        va = img[a]
        rows = [tile_sum(img[b] * va) for b in range(K + 1)]
        rows.append(jnp.zeros((GR - K - 1, Z), f32))
        gpart[a] = jnp.concatenate(rows, axis=0)
        return carry

    lax.fori_loop(0, K + 1, gram_part, 0)
    lane_g = lax.broadcasted_iota(jnp.int32, (GR, Z), 1)
    gram = jnp.zeros((GR, Z), f32)
    for a in range(K + 1):
        gram = jnp.where(lane_g == a, jnp.sum(gpart[a], axis=1, keepdims=True), gram)
    def extend_all():
        for c in second:
            wait_recv(c)
        assemble_zones(1)

        def extend(f, carry):
            assemble(fields.at[f, 0], img[f], bx.at[1], by.at[1], bc.at[1], f, f * X, f)
            fields[f, 1] = zone_field(f)
            return carry

        lax.fori_loop(0, K + 1, extend, 0)

    part = gram[:8]
    for q in range(1, GR // 8):
        part = part + pltpu.roll(gram[8 * q : 8 * q + 8], q * GW, 1)
    part = all_reduce(part, TWO, (gred1, gred2), 2, extend_all)
    gram = [part] + [pltpu.roll(part, Z - q * GW, 1) for q in range(1, GR // 8)]
    gram = jnp.concatenate(gram, axis=0)

    lane_k = lax.broadcasted_iota(jnp.int32, (K, Z), 1)
    row_k = lax.broadcasted_iota(jnp.int32, (K, Z), 0)
    a_mat = jnp.where(lane_k < K, gram[:K], 0.0)
    for k in range(K):
        prow = a_mat[k : k + 1, :]
        pcol = a_mat[:, k : k + 1]
        inv_p = 1.0 / a_mat[k : k + 1, k : k + 1]
        prow_s = jnp.where(lax.broadcasted_iota(jnp.int32, (1, Z), 1) == k, 1.0, prow) * inv_p
        base = jnp.where(lane_k == k, 0.0, a_mat)
        a_mat = jnp.where(row_k == k, jnp.broadcast_to(prow_s, (K, Z)), base - pcol * prow_s)
    mat[...] = jnp.where(lane2 == row2, 1.0, 0.0)
    mat[0:K, :] = a_mat
    grow = jnp.where(lax.broadcasted_iota(jnp.int32, (1, Z), 1) < K, gram[K : K + 1, :], 0.0)
    ecoef[...] = jnp.broadcast_to(jnp.sum(a_mat * grow, axis=1, keepdims=True), (K, Z))

    def begin(p, carry):
        z, x = lax.div(p, X + 2), lax.rem(p, X + 2)
        v = fields[C0, z, x]
        for a in range(K):
            v = v - ecoef[a : a + 1, :] * fields[a, z, x]
        fields[C0, z, x] = v
        return carry

    lax.fori_loop(0, 2 * (X + 2), begin, 0)
    for c in first + second:
        wait_send(c)
    hcols[...] = jnp.zeros((32, Z), f32)
    scale[...] = jnp.where(row2 < K, 1.0, 0.0)

    def step(j, carry):
        par = lax.rem(j, 2)
        u = fields[C0 + j, 0]
        w = apply(u, fields[C0 + j, 1])
        wbuf[par, 0] = w
        pack_faces(w, wface.at[par], wedge.at[par], 0, 0)
        cs = step_copies(par)

        @pl.when(j < STEPS - 1)
        def _():
            start_halo(cs)

        rows = [tile_sum(fields[f, 0, 1 : X + 1, 0:Y, :] * w) for f in range(K + STEPS)]
        ui = u[1 : X + 1, :Y]
        rows.append(tile_sum(w * w))
        rows.append(tile_sum(ui * ui))
        rows.append(jnp.zeros((32 - K - STEPS - 2, Z), f32))
        sums = jnp.sum(jnp.concatenate(rows, axis=0), axis=1, keepdims=True)
        part = jnp.sum(jnp.where(lane2 == row2, sums, 0.0), axis=0, keepdims=True)
        def extend_w():
            @pl.when(j < STEPS - 1)
            def _():
                wait_recv(cs)
                slot = 2 + par
                assemble(temp, wbuf[par, 0], mx.at[par], my.at[par], mc.at[par], 0, 0, 0)
                fields[C0 + 1 + j, 0] = temp[...]
                assemble_zones(slot)
                fields[C0 + 1 + j, 1] = jnp.where(
                    lane3 == Z - 1, zext[0], jnp.where(lane3 == 0, zext[1], 0.0)
                )

            @pl.when(j == STEPS - 1)
            def _():
                fields[C0 + STEPS, 0, 1 : X + 1, 0:Y, :] = wbuf[par, 0]

        total = all_reduce(part, groups, (sred1.at[par], sred2.at[par]), par, extend_w)
        c = jnp.broadcast_to(jnp.sum(mat[...] * total, axis=1, keepdims=True), (32, Z))
        uu = c[K + STEPS + 1 : K + STEPS + 2, :]
        sc = jnp.where(row2 == C0 + j, 1.0 / uu, scale[...])
        scale[...] = sc
        hcols[...] = jnp.where(lane2 == j, c, hcols[...])
        inv_n = 1.0 / jnp.sqrt(uu)
        coef[...] = jnp.where(
            row2 < K + STEPS, c * sc * inv_n, jnp.where(row2 == 30, inv_n, total)
        )

        def update(p, carry):
            z, x = lax.div(p, X + 2), lax.rem(p, X + 2)
            v = coef[30:31, :] * fields[C0 + 1 + j, z, x]
            v2 = jnp.zeros_like(v)
            for a in range(0, K + STEPS, 2):
                v = v - coef[a : a + 1, :] * fields[a, z, x]
                v2 = v2 - coef[a + 1 : a + 2, :] * fields[a + 1, z, x]
            fields[C0 + 1 + j, z, x] = v + v2
            return carry

        lax.fori_loop(0, 2 * (X + 2), update, 0)

        @pl.when(j < STEPS - 1)
        def _():
            wait_send(cs)

        return carry

    lax.fori_loop(0, STEPS, step, 0)

    lane8 = lane2[:8]
    row8 = row2[:8]
    hc = hcols[...]
    inv_n2 = scale[C0 : C0 + STEPS, :]
    inv_col = jnp.sqrt(inv_n2)
    n_col = 1.0 / inv_col
    inv_row = jnp.sum(jnp.where(lane8 == row8, inv_col, 0.0), axis=0, keepdims=True)
    last_c = jnp.sum(jnp.where(lane2 == STEPS - 1, hc, 0.0), axis=1, keepdims=True)
    raw = jnp.broadcast_to(coef[31:32, :], (32, Z))
    raw_col = jnp.sum(jnp.where(lane2 == row2, raw, 0.0), axis=1, keepdims=True)
    terms = jnp.where(row2[:, :1] < K + STEPS, raw_col * last_c * scale[:, :1], 0.0)
    used = jnp.sum(terms, axis=0, keepdims=True)
    last_sq = (raw_col[K + STEPS : K + STEPS + 1] - used) * inv_n2[STEPS - 1 : STEPS, :1]
    last_n = jnp.sqrt(last_sq)
    upper = hc[C0 : C0 + STEPS] * inv_col * inv_row
    upper = jnp.where(lane8 < STEPS, upper, 0.0)
    upper = jnp.where(lane8 == row8 - 1, n_col, upper)
    lane1 = lane2[:1]
    bottom = jnp.where(lane1 == STEPS - 1, last_n, 0.0)
    hes = jnp.concatenate([upper, bottom], axis=0)
    hes_out[...] = hes[:, :STEPS]

    rows = [hes[i : i + 1] for i in range(STEPS + 1)]
    rows[0] = jnp.where(lane1 == STEPS, n_col[0:1], rows[0])
    for i in range(STEPS):
        top, low = rows[i][:, i : i + 1], rows[i + 1][:, i : i + 1]
        inv_r = 1.0 / jnp.sqrt(top * top + low * low)
        cs_, sn = top * inv_r, low * inv_r
        rows[i], rows[i + 1] = cs_ * rows[i] + sn * rows[i + 1], cs_ * rows[i + 1] - sn * rows[i]
    ysol = jnp.zeros((1, Z), f32)
    for i in range(STEPS - 1, -1, -1):
        known = jnp.sum(jnp.where(lane1 > i, rows[i] * ysol, 0.0), axis=1, keepdims=True)
        yi = (rows[i][:, STEPS : STEPS + 1] - known) / rows[i][:, i : i + 1]
        ysol = jnp.where(lane1 == i, yi, ysol)

    rcoef = ecoef[:, :1] - jnp.sum(hc[:K] * (ysol * inv_row), axis=1, keepdims=True)
    ycol = jnp.sum(jnp.where(lane8 == row8, ysol * inv_row, 0.0), axis=1, keepdims=True)
    hy8 = jnp.sum(upper * ysol, axis=1, keepdims=True) * inv_col[:, :1]
    hy9 = jnp.sum(bottom * ysol, axis=1, keepdims=True) / last_n
    out = guess[...]
    for a in range(K):
        out = out + rcoef[a : a + 1, :] * rec[a]
    res = fields[C0, 0, 1 : X + 1, 0:Y, :]
    for i in range(STEPS):
        ui = fields[C0 + i, 0, 1 : X + 1, 0:Y, :]
        out = out + ycol[i : i + 1, :] * ui
        res = res - hy8[i : i + 1, :] * ui
    res = res - hy9 * fields[C0 + STEPS, 0, 1 : X + 1, 0:Y, :]
    sol_out[...] = out
    res_out[...] = res


def round_up(n, m):
    return (n + m - 1) // m * m


def solution(mesh):
    sizes = tuple(mesh.shape[a] for a in AXES)

    def body(right_side, start_guess, conductivity, recycled):
        K, X, Y, Z = recycled.shape
        NF = K + 2
        FR, ER, XR = round_up(NF * X, 8), round_up(NF, 8), round_up(X, 8)
        def count(group):
            n = 1
            for a in group:
                n *= mesh.shape[a]
            return n

        groups = ONE if count(AXES) <= 64 else TWO
        n_two, n_step = [count(g) for g in TWO], [count(g) for g in groups]
        biggest = max(n_two + n_step)
        nc = (NF + CHUNK - 1) // CHUNK
        GR = round_up(K + 1, 8)
        V = lambda *s: pltpu.VMEM(s, jnp.float32)
        vm = pl.BlockSpec(memory_space=pltpu.VMEM)
        shape = jax.ShapeDtypeStruct((X, Y, Z), jnp.float32)
        return pl.pallas_call(
            functools.partial(kernel, sizes, groups),
            out_shape=(shape, shape, jax.ShapeDtypeStruct((STEPS + 1, STEPS), jnp.float32)),
            in_specs=[vm] * 4,
            out_specs=(vm, vm, vm),
            scratch_shapes=[
                V(NF, X, Y, Z), V(NF, X, Y, Z),
                V(2, 2, FR, Z), V(2, 2, 2, ER, Z),
                V(2, 2, 1, X, Y, Z), V(2, 2, 2, XR, Z), V(2, 2, 2, 2, 1, Z),
                V(2, 2, NF, Y, Z), V(2, 2, FR, Z), V(2, 2, 2, ER, Z),
                V(4, 2, 1, X, Y, Z), V(4, 2, 2, 1, Y, Z), V(4, 2, 2, XR, Z), V(4, 2, 2, 2, 1, Z),
                V(2, 2, 1, Y, Z), V(2, 2, XR, Z), V(2, 2, 2, 1, Z),
                V(2, 1, X, Y, Z), V(2, 2, XR, Z), V(2, 2, 2, 1, Z),
                V(K + STEPS + 1, 2, X + 2, Y + 8, Z), V(2, X + 2, Y + 8, Z), V(X, Y, Z),
                V(X + 2, Y + 8, Z), V(2, X + 2, Y + 8, Z),
                V(K + 1, GR, Z), V(n_two[0], 8, Z), V(n_two[1], 8, Z),
                V(2, n_step[0], 1, Z), V(2, n_step[-1], 1, Z),
                V(32, Z), V(32, Z), V(32, Z), V(32, Z), V(K, Z),
                pltpu.SemaphoreType.DMA((2 * nc + 4, 26)), pltpu.SemaphoreType.DMA((2 * nc + 4, 26)),
                pltpu.SemaphoreType.DMA((3, 2, biggest)), pltpu.SemaphoreType.DMA((3, 2, biggest)),
            ],
            compiler_params=pltpu.CompilerParams(collective_id=0, has_side_effects=True),
        )(right_side, start_guess, conductivity, recycled)

    return jax.shard_map(
        body,
        mesh=mesh,
        in_specs=(P(*AXES), P(*AXES), P(*AXES), P(None, *AXES)),
        out_specs=(P(*AXES), P(*AXES), P()),
        check_vma=False,
    )
```

```python
import functools
import itertools

import jax
import jax.numpy as jnp
from jax import lax
from jax.experimental import pallas as pl
from jax.experimental.pallas import tpu as pltpu
from jax.sharding import PartitionSpec as P

STEPS = 8
MESH = pl.DeviceIdType.MESH
AXES = ("px", "py", "pz")
TWO = (("py", "pz"), ("px",))
ONE = (("px", "py", "pz"),)
CHUNK = 8

edge_weight = 0.25 ** (1.0 / 3.0)
middle_weight = 2.0 * edge_weight
shift_value = 0.4

DIRS = [d for d in itertools.product((-1, 0, 1), repeat=3) if d != (0, 0, 0)]


def kernel(
    sizes, groups,
    rhs, guess, cond, rec,
    sol_out, res_out, hes_out,
    src, img, bface, bedge, pack, pface, pedge,
    bx, by, bc,
    zm, zx, zy, zc,
    mx, my, mc,
    wbuf, wface, wedge,
    fields, kext, diag, temp, zext,
    gpart, gred1, gred2, sred1, sred2,
    mat, hcols, scale, coef, ecoef,
    hsend, hrecv, rsend, rrecv,
):
    nsz = dict(zip(AXES, sizes))
    me = {a: lax.axis_index(a) for a in AXES}
    K, X, Y, Z = rec.shape
    NF = K + 2
    C0 = K
    f32 = jnp.float32
    lane3 = lax.broadcasted_iota(jnp.int32, (X + 2, Y + 8, Z), 2)
    lane2 = lax.broadcasted_iota(jnp.int32, (32, Z), 1)
    row2 = lax.broadcasted_iota(jnp.int32, (32, Z), 0)

    def exists(d):
        ok = None
        for a, s in zip(AXES, d):
            if s == 0:
                continue
            here = (me[a] < nsz[a] - 1) if s > 0 else (me[a] > 0)
            ok = here if ok is None else jnp.logical_and(ok, here)
        return ok

    def possible(d):
        return all(s == 0 or nsz[a] > 1 for a, s in zip(AXES, d))

    dirs = [(i, d) for i, d in enumerate(DIRS) if possible(d)]

    def target(d):
        return tuple(me[a] + s for a, s in zip(AXES, d))

    def group_info(group):
        n = 1
        rank = 0
        for a in group:
            n *= nsz[a]
            rank = rank * nsz[a] + me[a]
        return n, rank

    def member(group, r):
        co = dict(me)
        for a in reversed(group):
            co[a] = lax.rem(r, nsz[a])
            r = lax.div(r, nsz[a])
        return tuple(co[a] for a in AXES)

    def copies(sends, recvs, slot, zones):
        out = []
        for i, (dx, dy, dz) in dirs:
            if (dz != 0) not in zones:
                continue
            main, face, edge = sends(dz)
            rm, rx, ry, rc = recvs(-dz)
            hx, hy = int(dx > 0), int(dy > 0)
            if dx == 0 and dy == 0:
                s, t = main, rm
            elif dy == 0:
                s, t = main.at[:, X - 1 if hx else 0], rx.at[1 - hx]
            elif dx == 0:
                s, t = face.at[hy], ry.at[1 - hy]
            else:
                s, t = edge.at[hx, hy], rc.at[1 - hx, 1 - hy]
            d = (dx, dy, dz)
            out.append((d, pltpu.make_async_remote_copy(
                src_ref=s, dst_ref=t,
                send_sem=hsend.at[slot, i], recv_sem=hrecv.at[slot, i],
                device_id=target(d), device_id_type=MESH,
            )))
        return out

    def start_halo(cs):
        for d, c in cs:
            pl.when(exists(d))(c.start)

    def wait_recv(cs):
        for d, c in cs:
            pl.when(exists(tuple(-s for s in d)))(c.wait_recv)

    def wait_send(cs):
        for d, c in cs:
            pl.when(exists(d))(c.wait_send)

    NC = (NF + CHUNK - 1) // CHUNK

    def batch_copies(b, c):
        f0, f1 = c * CHUNK, min((c + 1) * CHUNK, NF)
        fs, es = pl.ds(f0, f1 - f0), pl.ds(f0, CHUNK)
        rows = pl.ds(f0 * X, min(CHUNK * X, bface.shape[2] - f0 * X))

        def sends(dz):
            if dz == 0:
                body = (src if b == 0 else img).at[fs]
                return body, bface.at[b, :, rows], bedge.at[b, :, :, es]
            h = int(dz > 0)
            return pack.at[b, h], pface.at[b, h], pedge.at[b, h]

        def recvs(z):
            if z == 0:
                return None, bx.at[b, :, fs], by.at[b, :, rows], bc.at[b, :, :, es]
            h = int(z > 0)
            return zm.at[b, h], zx.at[b, h], zy.at[b, h], zc.at[b, h]

        return copies(sends, recvs, b * (NC + 1) + c, (c == NC,))

    def step_copies(par):
        def sends(dz):
            return wbuf.at[par], wface.at[par], wedge.at[par]

        def recvs(z):
            if z == 0:
                return None, mx.at[par], my.at[par], mc.at[par]
            h = int(z > 0)
            return zm.at[2 + par, h], zx.at[2 + par, h], zy.at[2 + par, h], zc.at[2 + par, h]

        return copies(sends, recvs, 2 * (NC + 1) + par, (False, True))

    def pack_faces(val, face, edge, row, erow):
        for h, y in ((0, 0), (1, Y - 1)):
            for x in range(X):
                face[h, pl.ds(row + x, 1), :] = val[x, y : y + 1, :]
            edge[0, h, pl.ds(erow, 1), :] = val[0, y : y + 1, :]
            edge[1, h, pl.ds(erow, 1), :] = val[X - 1, y : y + 1, :]

    def assemble(dst, main, rx, ry, rc, f, row, erow):
        dst[1 : X + 1, 0:Y, :] = main
        dst[0, 0:Y, :] = rx[0, f]
        dst[X + 1, 0:Y, :] = rx[1, f]
        for h, y in ((1, Y), (0, Y + 7)):
            for x in range(X):
                dst[1 + x, y : y + 1, :] = ry[h, pl.ds(row + x, 1), :]
            dst[0, y : y + 1, :] = rc[0, h, pl.ds(erow, 1), :]
            dst[X + 1, y : y + 1, :] = rc[1, h, pl.ds(erow, 1), :]

    def assemble_zones(slot):
        for h in range(2):
            assemble(zext.at[h], zm[slot, h, 0], zx.at[slot, h], zy.at[slot, h], zc.at[slot, h], 0, 0, 0)

    def zone_field(f):
        low = pltpu.roll(zext[0], lax.rem(2 * Z - 1 - f, Z), 2)
        high = pltpu.roll(zext[1], lax.rem(Z - f, Z), 2)
        return jnp.where(lane3 == Z - 1, low, jnp.where(lane3 == 0, high, 0.0))

    def pack_lanes(get, count, b):
        lane = lax.broadcasted_iota(jnp.int32, (X, Y, Z), 2)
        low = jnp.zeros((X, Y, Z), f32)
        high = jnp.zeros((X, Y, Z), f32)
        for f in range(count):
            v = get(f)
            low = jnp.where(lane == f, pltpu.roll(v, f, 2) if f else v, low)
            high = jnp.where(lane == f, pltpu.roll(v, (f + 1) % Z, 2), high)
        for h, v in ((0, low), (1, high)):
            pack[b, h, 0] = v
            pack_faces(v, pface.at[b, h], pedge.at[b, h], 0, 0)

    def stencil(e, b):
        left = pltpu.roll(jnp.where(lane3 == Z - 1, b, e), 1, 2)
        right = pltpu.roll(jnp.where(lane3 == 0, b, e), Z - 1, 2)
        az = edge_weight * (left + right) + middle_weight * e
        ay = edge_weight * (pltpu.roll(az, 1, 1) + pltpu.roll(az, Y + 7, 1)) + middle_weight * az
        ay = ay[:, :Y]
        ax = edge_weight * (ay[:X] + ay[2:]) + middle_weight * ay[1 : X + 1]
        return ax - 2.0 * e[1 : X + 1, :Y]

    def apply(e, b):
        k = kext[0]
        near = stencil(e, b)
        far = stencil(k * e, kext[1] * b)
        return diag[...] * e[1 : X + 1, :Y] - 0.5 * k[1 : X + 1, :Y] * near - 0.5 * far

    def tile_sum(v):
        v = jnp.sum(v.reshape(X * Y // 8, 8, Z), axis=0)
        return jnp.sum(v, axis=0, keepdims=True)

    def all_reduce(value, groups, bufs, slot, between):
        total = value
        for g, group in enumerate(groups):
            n, rank = group_info(group)
            buf = bufs[g]
            buf[rank] = total
            cs = []
            for k in sorted(range(1, n), key=lambda k: -min(k, n - k)):
                c = pltpu.make_async_remote_copy(
                    src_ref=buf.at[rank], dst_ref=buf.at[rank],
                    send_sem=rsend.at[slot, g, k], recv_sem=rrecv.at[slot, g, k],
                    device_id=member(group, lax.rem(rank + k, n)), device_id_type=MESH,
                )
                c.start()
                cs.append((k, c))
            if g == len(groups) - 1:
                between()
            for k, c in cs:
                pltpu.make_async_remote_copy(
                    src_ref=buf.at[rank], dst_ref=buf.at[lax.rem(rank + n - k, n)],
                    send_sem=rsend.at[slot, g, k], recv_sem=rrecv.at[slot, g, k],
                    device_id=member(group, lax.rem(rank + k, n)), device_id_type=MESH,
                ).wait_recv()
            parts = [buf[r] for r in range(n)]
            while len(parts) > 1:
                parts = [sum(parts[r : r + 2][1:], parts[r]) for r in range(0, len(parts), 2)]
            total = parts[0]
            for k, c in cs:
                c.wait_send()
        return total

    def clear_all(refs):
        for ref in refs:
            def clear(i, carry, ref=ref):
                ref[i] = jnp.zeros(ref.shape[1:], f32)
                return carry

            lax.fori_loop(0, ref.shape[0], clear, 0)

    clear_all((bx, by, bc, zm, zx, zy, zc, mx, my, mc))
    barrier = pltpu.get_barrier_semaphore()
    count = jnp.int32(0)
    for _, d in dirs:
        ok = exists(d)

        @pl.when(ok)
        def _(d=d):
            pl.semaphore_signal(barrier, inc=1, device_id=target(d), device_id_type=MESH)

        count = count + ok.astype(jnp.int32)
    for group in TWO:
        n, rank = group_info(group)
        for k in range(1, n):
            pl.semaphore_signal(
                barrier, inc=1, device_id=member(group, lax.rem(rank + k, n)), device_id_type=MESH
            )
        count = count + (n - 1)

    clear_all((wface, wedge, bface, bedge, pface, pedge))

    def load_field(f, carry):
        v = rec[f]
        src[f] = v
        pack_faces(v, bface.at[0], bedge.at[0], f * X, f)
        return carry

    lax.fori_loop(0, K, load_field, 0)
    for f, ref in ((K, guess), (K + 1, cond)):
        v = ref[...]
        src[f] = v
        pack_faces(v, bface.at[0], bedge.at[0], f * X, f)
    pack_lanes(lambda f: src[f], NF, 0)
    pl.semaphore_wait(barrier, count)

    first = [batch_copies(0, c) for c in range(NC + 1)]
    second = [batch_copies(1, c) for c in range(NC + 1)]
    order = [NC - 1] + list(range(NC - 1))
    for c in [NC] + order:
        start_halo(first[c])
    clear_all((fields, kext, zext))
    temp[...] = jnp.zeros(temp.shape, f32)
    img[NF - 1] = jnp.zeros((X, Y, Z), f32)
    wait_recv(first[NC])
    assemble_zones(0)

    def image(f, carry):
        assemble(temp, src[f], bx.at[0], by.at[0], bc.at[0], f, f * X, f)
        v = apply(temp[...], zone_field(f))
        img[f] = v
        pack_faces(v, bface.at[1], bedge.at[1], f * X, f)
        return carry

    for c in order:
        wait_recv(first[c])
        if c == NC - 1:
            assemble(kext.at[0], src[K + 1], bx.at[0], by.at[0], bc.at[0], K + 1, (K + 1) * X, K + 1)
            kext[1] = zone_field(K + 1)
            k_all = kext[0]
            diag[...] = shift_value + 7.0 * k_all[1 : X + 1, :Y] + 0.5 * stencil(k_all, kext[1])
            lax.fori_loop(c * CHUNK, K + 1, image, 0)
            v = rhs[...] - img[K]
            img[K] = v
            pack_faces(v, bface.at[1], bedge.at[1], K * X, K)
        else:
            lax.fori_loop(c * CHUNK, (c + 1) * CHUNK, image, 0, unroll=2)
        start_halo(second[c])
    pack_lanes(lambda f: img[f], K + 1, 1)
    start_halo(second[NC])

    GR = gpart.shape[1]
    GW = Z // (GR // 8)
    assert K + 1 <= GW

    def gram_part(a, carry):
        va = img[a]
        rows = [tile_sum(img[b] * va) for b in range(K + 1)]
        rows.append(jnp.zeros((GR - K - 1, Z), f32))
        gpart[a] = jnp.concatenate(rows, axis=0)
        return carry

    lax.fori_loop(0, K + 1, gram_part, 0, unroll=2)
    lane_g = lax.broadcasted_iota(jnp.int32, (GR, Z), 1)
    gram = jnp.zeros((GR, Z), f32)
    for a in range(K + 1):
        gram = jnp.where(lane_g == a, jnp.sum(gpart[a], axis=1, keepdims=True), gram)
    def extend_all():
        for c in second:
            wait_recv(c)
        assemble_zones(1)

        def extend(f, carry):
            assemble(fields.at[f, 0], img[f], bx.at[1], by.at[1], bc.at[1], f, f * X, f)
            fields[f, 1] = zone_field(f)
            return carry

        lax.fori_loop(0, K + 1, extend, 0, unroll=4)

    part = gram[:8]
    for q in range(1, GR // 8):
        part = part + pltpu.roll(gram[8 * q : 8 * q + 8], q * GW, 1)
    part = all_reduce(part, TWO, (gred1, gred2), 2, extend_all)
    gram = [part] + [pltpu.roll(part, Z - q * GW, 1) for q in range(1, GR // 8)]
    gram = jnp.concatenate(gram, axis=0)

    lane_k = lax.broadcasted_iota(jnp.int32, (K, Z), 1)
    row_k = lax.broadcasted_iota(jnp.int32, (K, Z), 0)
    a_mat = jnp.where(lane_k < K, gram[:K], 0.0)
    for k in range(K):
        prow = a_mat[k : k + 1, :]
        pcol = a_mat[:, k : k + 1]
        inv_p = 1.0 / a_mat[k : k + 1, k : k + 1]
        prow_s = jnp.where(lax.broadcasted_iota(jnp.int32, (1, Z), 1) == k, 1.0, prow) * inv_p
        base = jnp.where(lane_k == k, 0.0, a_mat)
        a_mat = jnp.where(row_k == k, jnp.broadcast_to(prow_s, (K, Z)), base - pcol * prow_s)
    mat[...] = jnp.where(lane2 == row2, 1.0, 0.0)
    mat[0:K, :] = a_mat
    grow = jnp.where(lax.broadcasted_iota(jnp.int32, (1, Z), 1) < K, gram[K : K + 1, :], 0.0)
    ecoef[...] = jnp.broadcast_to(jnp.sum(a_mat * grow, axis=1, keepdims=True), (K, Z))

    def begin(p, carry):
        z, x = lax.div(p, X + 2), lax.rem(p, X + 2)
        v = fields[C0, z, x]
        for a in range(K):
            v = v - ecoef[a : a + 1, :] * fields[a, z, x]
        fields[C0, z, x] = v
        return carry

    lax.fori_loop(0, 2 * (X + 2), begin, 0)
    for c in first + second:
        wait_send(c)
    hcols[...] = jnp.zeros((32, Z), f32)
    scale[...] = jnp.where(row2 < K, 1.0, 0.0)

    def step(j, carry):
        par = lax.rem(j, 2)
        u = fields[C0 + j, 0]
        w = apply(u, fields[C0 + j, 1])
        wbuf[par, 0] = w
        pack_faces(w, wface.at[par], wedge.at[par], 0, 0)
        cs = step_copies(par)

        @pl.when(j < STEPS - 1)
        def _():
            start_halo(cs)

        rows = [tile_sum(fields[f, 0, 1 : X + 1, 0:Y, :] * w) for f in range(K + STEPS)]
        ui = u[1 : X + 1, :Y]
        rows.append(tile_sum(w * w))
        rows.append(tile_sum(ui * ui))
        rows.append(jnp.zeros((32 - K - STEPS - 2, Z), f32))
        sums = jnp.sum(jnp.concatenate(rows, axis=0), axis=1, keepdims=True)
        part = jnp.sum(jnp.where(lane2 == row2, sums, 0.0), axis=0, keepdims=True)
        def extend_w():
            @pl.when(j < STEPS - 1)
            def _():
                wait_recv(cs)
                slot = 2 + par
                assemble(temp, wbuf[par, 0], mx.at[par], my.at[par], mc.at[par], 0, 0, 0)
                fields[C0 + 1 + j, 0] = temp[...]
                assemble_zones(slot)
                fields[C0 + 1 + j, 1] = jnp.where(
                    lane3 == Z - 1, zext[0], jnp.where(lane3 == 0, zext[1], 0.0)
                )

            @pl.when(j == STEPS - 1)
            def _():
                fields[C0 + STEPS, 0, 1 : X + 1, 0:Y, :] = wbuf[par, 0]

        total = all_reduce(part, groups, (sred1.at[par], sred2.at[par]), par, extend_w)
        c = jnp.broadcast_to(jnp.sum(mat[...] * total, axis=1, keepdims=True), (32, Z))
        uu = c[K + STEPS + 1 : K + STEPS + 2, :]
        sc = jnp.where(row2 == C0 + j, 1.0 / uu, scale[...])
        scale[...] = sc
        hcols[...] = jnp.where(lane2 == j, c, hcols[...])
        inv_n = 1.0 / jnp.sqrt(uu)
        coef[...] = jnp.where(
            row2 < K + STEPS, c * sc * inv_n, jnp.where(row2 == 30, inv_n, total)
        )

        def update(p, carry):
            z, x = lax.div(p, X + 2), lax.rem(p, X + 2)
            v = coef[30:31, :] * fields[C0 + 1 + j, z, x]
            v2 = jnp.zeros_like(v)
            for a in range(0, K + STEPS, 2):
                v = v - coef[a : a + 1, :] * fields[a, z, x]
                v2 = v2 - coef[a + 1 : a + 2, :] * fields[a + 1, z, x]
            fields[C0 + 1 + j, z, x] = v + v2
            return carry

        lax.fori_loop(0, 2 * (X + 2), update, 0, unroll=4)

        @pl.when(j < STEPS - 1)
        def _():
            wait_send(cs)

        return carry

    lax.fori_loop(0, STEPS, step, 0)

    lane8 = lane2[:8]
    row8 = row2[:8]
    hc = hcols[...]
    inv_n2 = scale[C0 : C0 + STEPS, :]
    inv_col = jnp.sqrt(inv_n2)
    n_col = 1.0 / inv_col
    inv_row = jnp.sum(jnp.where(lane8 == row8, inv_col, 0.0), axis=0, keepdims=True)
    last_c = jnp.sum(jnp.where(lane2 == STEPS - 1, hc, 0.0), axis=1, keepdims=True)
    raw = jnp.broadcast_to(coef[31:32, :], (32, Z))
    raw_col = jnp.sum(jnp.where(lane2 == row2, raw, 0.0), axis=1, keepdims=True)
    terms = jnp.where(row2[:, :1] < K + STEPS, raw_col * last_c * scale[:, :1], 0.0)
    used = jnp.sum(terms, axis=0, keepdims=True)
    last_sq = (raw_col[K + STEPS : K + STEPS + 1] - used) * inv_n2[STEPS - 1 : STEPS, :1]
    last_n = jnp.sqrt(last_sq)
    upper = hc[C0 : C0 + STEPS] * inv_col * inv_row
    upper = jnp.where(lane8 < STEPS, upper, 0.0)
    upper = jnp.where(lane8 == row8 - 1, n_col, upper)
    lane1 = lane2[:1]
    bottom = jnp.where(lane1 == STEPS - 1, last_n, 0.0)
    hes = jnp.concatenate([upper, bottom], axis=0)
    hes_out[...] = hes[:, :STEPS]

    rows = [hes[i : i + 1] for i in range(STEPS + 1)]
    rows[0] = jnp.where(lane1 == STEPS, n_col[0:1], rows[0])
    for i in range(STEPS):
        top, low = rows[i][:, i : i + 1], rows[i + 1][:, i : i + 1]
        inv_r = 1.0 / jnp.sqrt(top * top + low * low)
        cs_, sn = top * inv_r, low * inv_r
        rows[i], rows[i + 1] = cs_ * rows[i] + sn * rows[i + 1], cs_ * rows[i + 1] - sn * rows[i]
    ysol = jnp.zeros((1, Z), f32)
    for i in range(STEPS - 1, -1, -1):
        known = jnp.sum(jnp.where(lane1 > i, rows[i] * ysol, 0.0), axis=1, keepdims=True)
        yi = (rows[i][:, STEPS : STEPS + 1] - known) / rows[i][:, i : i + 1]
        ysol = jnp.where(lane1 == i, yi, ysol)

    rcoef = ecoef[:, :1] - jnp.sum(hc[:K] * (ysol * inv_row), axis=1, keepdims=True)
    ycol = jnp.sum(jnp.where(lane8 == row8, ysol * inv_row, 0.0), axis=1, keepdims=True)
    hy8 = jnp.sum(upper * ysol, axis=1, keepdims=True) * inv_col[:, :1]
    hy9 = jnp.sum(bottom * ysol, axis=1, keepdims=True) / last_n
    out = guess[...]
    for a in range(K):
        out = out + rcoef[a : a + 1, :] * rec[a]
    res = fields[C0, 0, 1 : X + 1, 0:Y, :]
    for i in range(STEPS):
        ui = fields[C0 + i, 0, 1 : X + 1, 0:Y, :]
        out = out + ycol[i : i + 1, :] * ui
        res = res - hy8[i : i + 1, :] * ui
    res = res - hy9 * fields[C0 + STEPS, 0, 1 : X + 1, 0:Y, :]
    sol_out[...] = out
    res_out[...] = res


def deliver(sol, res, hes, sol_out, res_out, hes_out):
    sol_out[...] = sol[...]
    res_out[...] = res[...]
    hes_out[...] = hes[...]


def round_up(n, m):
    return (n + m - 1) // m * m


def solution(mesh):
    sizes = tuple(mesh.shape[a] for a in AXES)

    def body(right_side, start_guess, conductivity, recycled):
        K, X, Y, Z = recycled.shape
        NF = K + 2
        FR, ER, XR = round_up(NF * X, 8), round_up(NF, 8), round_up(X, 8)
        def count(group):
            n = 1
            for a in group:
                n *= mesh.shape[a]
            return n

        groups = ONE if count(AXES) <= 64 else TWO
        n_two, n_step = [count(g) for g in TWO], [count(g) for g in groups]
        biggest = max(n_two + n_step)
        nc = (NF + CHUNK - 1) // CHUNK
        GR = round_up(K + 1, 8)
        V = lambda *s: pltpu.VMEM(s, jnp.float32)
        vm = pl.BlockSpec(memory_space=pltpu.VMEM)
        shape = jax.ShapeDtypeStruct((X, Y, Z), jnp.float32)
        sol, res, hes = pl.pallas_call(
            functools.partial(kernel, sizes, groups),
            out_shape=(shape, shape, jax.ShapeDtypeStruct((STEPS + 1, STEPS), jnp.float32)),
            in_specs=[vm] * 4,
            out_specs=(vm, vm, vm),
            scratch_shapes=[
                V(NF, X, Y, Z), V(NF, X, Y, Z),
                V(2, 2, FR, Z), V(2, 2, 2, ER, Z),
                V(2, 2, 1, X, Y, Z), V(2, 2, 2, XR, Z), V(2, 2, 2, 2, 1, Z),
                V(2, 2, NF, Y, Z), V(2, 2, FR, Z), V(2, 2, 2, ER, Z),
                V(4, 2, 1, X, Y, Z), V(4, 2, 2, 1, Y, Z), V(4, 2, 2, XR, Z), V(4, 2, 2, 2, 1, Z),
                V(2, 2, 1, Y, Z), V(2, 2, XR, Z), V(2, 2, 2, 1, Z),
                V(2, 1, X, Y, Z), V(2, 2, XR, Z), V(2, 2, 2, 1, Z),
                V(K + STEPS + 1, 2, X + 2, Y + 8, Z), V(2, X + 2, Y + 8, Z), V(X, Y, Z),
                V(X + 2, Y + 8, Z), V(2, X + 2, Y + 8, Z),
                V(K + 1, GR, Z), V(n_two[0], 8, Z), V(n_two[1], 8, Z),
                V(2, n_step[0], 1, Z), V(2, n_step[-1], 1, Z),
                V(32, Z), V(32, Z), V(32, Z), V(32, Z), V(K, Z),
                pltpu.SemaphoreType.DMA((2 * nc + 4, 26)), pltpu.SemaphoreType.DMA((2 * nc + 4, 26)),
                pltpu.SemaphoreType.DMA((3, 2, biggest)), pltpu.SemaphoreType.DMA((3, 2, biggest)),
            ],
            compiler_params=pltpu.CompilerParams(collective_id=0, has_side_effects=True),
        )(right_side, start_guess, conductivity, recycled)
        return pl.pallas_call(
            deliver,
            out_shape=(shape, shape, jax.ShapeDtypeStruct(hes.shape, hes.dtype)),
            in_specs=[vm] * 3,
            out_specs=(vm,) * 3,
        )(sol, res, hes)

    return jax.shard_map(
        body,
        mesh=mesh,
        in_specs=(P(*AXES), P(*AXES), P(*AXES), P(None, *AXES)),
        out_specs=(P(*AXES), P(*AXES), P()),
        check_vma=False,
    )
```
